32 devices in a mesh: view: 4 (over x, core), pencil: 8 (over z, y).
Axes of the slice: x: 2, y: 2, z: 4, core: 2. Of those that a mesh axis runs over, the one named last changes fastest.
Arguments:
- recorded: float32 [4, 256, 256, 256], P('view', 'pencil'), may hold values from 0.5 to 4
- spectral_weight: float32 [4, 256, 256, 256], P('view', None, 'pencil'), may hold values from 0.05 to 1
- psf_taps: float32 [4, 3, 9], replicated, may hold values from 0.1 to 1
Outputs:
- joined_volume: float32 [256, 256, 256], P('pencil', 'view')
- estimate: float32 [256, 256, 256], P('pencil', 'view')
The draws below stay inside these ranges and needn't reach their ends.
All inputs are finite; a program needn't handle non-finite values.
Results may differ from the reference program's by a relative error of at most 0.00029.
Values sent between devices are 32-bit elements; how exact they have to be, the bound alone decides.
A program may use at most 192 MiB of HBM per device.

```python
import math
import jax
import jax.numpy as jnp
from jax import lax

NZ = 256
NY = 256
NX = 256
TAPS = 9
ITERS = 2
VIEWS = 4


def level_of(own_key, shape, pieces, low, top_value):
    level = 1.0
    for axis_at, blocks in pieces:
        draws = jax.random.uniform(jax.random.fold_in(jax.random.fold_in(own_key, 6), axis_at), (blocks,), jnp.float32, low / len(pieces), top_value / len(pieces))
        level = level * jnp.repeat(jnp.exp(draws), shape[axis_at] // blocks).reshape((-1,) + (1,) * (len(shape) - 1 - axis_at))
    return level


def setup_inputs(seed: int = 0) -> dict:
    arg_keys = jax.random.split(jax.random.key(seed), 4)
    return {
        "recorded": jnp.clip(jnp.exp(math.log(4.0) - 2.0794415 * jax.random.uniform(arg_keys[0], (VIEWS, NZ, NY, NX), jnp.float32) ** level_of(arg_keys[0], (VIEWS, NZ, NY, NX), ((0, 4), (1, 8)), -0.2, 0.2)), 0.5, 4.0),
        "spectral_weight": jnp.clip(jnp.exp(math.log(1.0) - 2.9957323 * jax.random.uniform(arg_keys[1], (VIEWS, NZ, NY, NX), jnp.float32) ** level_of(arg_keys[1], (VIEWS, NZ, NY, NX), ((0, 4), (2, 8)), -0.2, 0.2)), 0.05, 1.0),
        "psf_taps": jnp.clip(jnp.exp(jax.random.uniform(arg_keys[2], (VIEWS, 3, TAPS), jnp.float32, math.log(0.1), math.log(1.0))), 0.1, 1.0),
    }


def conv_along(field, column, axis_dim, margin):
    padding = [(0, 0)] * field.ndim
    padding[axis_dim] = (margin, margin)
    padded = jnp.pad(field, padding)
    length = field.shape[axis_dim]
    running = column[0] * lax.slice_in_dim(padded, 0, length, axis=axis_dim)
    for offset in range(1, column.shape[0]):
        running = running + column[offset] * lax.slice_in_dim(padded, offset, offset + length, axis=axis_dim)
    return running


def blur_field(field, kernel, margin):
    for axis_dim in range(3):
        field = conv_along(field, kernel[axis_dim], axis_dim, margin)
    return field


def reference(recorded, spectral_weight, psf_taps):
    combined = spectral_weight[0] * jnp.fft.fftn(recorded[0])
    for viewer in range(1, VIEWS):
        combined = combined + spectral_weight[viewer] * jnp.fft.fftn(recorded[viewer])
    joined_volume = jnp.real(jnp.fft.ifftn(combined)).astype(jnp.float32)
    kernels = psf_taps / jnp.sum(psf_taps, axis=-1, keepdims=True)
    margin = TAPS // 2
    estimate = 0.1 + jax.nn.softplus(joined_volume)
    for repeat in range(ITERS):
        summed = jnp.zeros_like(estimate)
        for viewer in range(VIEWS):
            blurred = blur_field(estimate, kernels[viewer], margin)
            ratio = recorded[viewer] / blurred
            summed = summed + blur_field(ratio, kernels[viewer][:, ::-1], margin)
        estimate = estimate * summed / VIEWS
    return joined_volume, estimate
```

```python
import functools
import math

import jax
import jax.numpy as jnp
from jax import lax
from jax.experimental import pallas as pl
from jax.experimental.pallas import tpu as pltpu
from jax.sharding import PartitionSpec as P

ITERS = 2
MESH = pl.DeviceIdType.MESH


def mix(form, left, right):
    return jnp.einsum(form, left, right, precision=lax.Precision.HIGH)


def turns(first, second, length):
    product = first[:, None] * second[None, :] % length
    phases = product.astype(jnp.float32) * (2.0 * math.pi / length)
    return (jnp.cos(phases), jnp.sin(phases))


def rotation(cos, sin):
    return jnp.stack([jnp.stack([cos, sin]), jnp.stack([-sin, cos])])


def exchange(parts, axis):
    count = len(parts)
    got = [parts[0]]
    for step in range(1, count):
        pairs = [(i, (i + step) % count) for i in range(count)]
        got.append(lax.ppermute(parts[step], axis, pairs))
    return got


def flat_rows(value, width):
    flat = value.reshape(-1)
    rest = -flat.shape[0] % width
    return jnp.pad(flat, (0, rest)).reshape(-1, width)


def padded_2(shard, sides, width):
    for axis, dim in sides:
        devices, length = (lax.axis_size(axis), shard.shape[dim])
        up = [(i, (i + 1) % devices) for i in range(devices - 1)]
        down = [(j, i) for i, j in up]
        last = lax.slice_in_dim(shard, length - width, length, axis=dim)
        leading = lax.slice_in_dim(shard, 0, width, axis=dim)
        before = lax.ppermute(last, axis, up)
        after = lax.ppermute(leading, axis, down)
        shard = jnp.concatenate([before, shard, after], axis=dim)
    return shard


def folded(full, axis, dim, width):
    devices, length = (lax.axis_size(axis), full.shape[dim] - 2 * width)
    up = [(i, (i + 1) % devices) for i in range(devices - 1)]
    down = [(j, i) for i, j in up]
    before = lax.slice_in_dim(full, 0, width, axis=dim)
    after = lax.slice_in_dim(full, length + width, length + 2 * width, axis=dim)
    own = lax.slice_in_dim(full, width, length + width, axis=dim)
    from_below = lax.ppermute(after, axis, up)
    from_above = lax.ppermute(before, axis, down)
    spread = [(0, 0, 0)] * full.ndim
    spread[dim] = (0, length - width, 0)
    lower = lax.pad(from_below, jnp.float32(0), spread)
    spread[dim] = (length - width, 0, 0)
    return own + lower + lax.pad(from_above, jnp.float32(0), spread)


def band(taps, rows, columns, shift):
    offset = jnp.arange(columns)[None, :] - jnp.arange(rows)[:, None] + shift
    total = jnp.zeros((taps.shape[0], rows, columns), jnp.float32)
    for t in range(taps.shape[1]):
        total = total + jnp.where(offset == t, taps[:, t, None, None], 0.0)
    return total


def parts_of(value):
    high = lax.reduce_precision(value, 8, 7)
    return high.astype(jnp.bfloat16), (value - high).astype(jnp.bfloat16)


def thrice(table_high, table_low, value):
    high = value.astype(jnp.bfloat16)
    low = (value - high.astype(jnp.float32)).astype(jnp.bfloat16)
    total = jnp.dot(table_high, high, preferred_element_type=jnp.float32)
    total += jnp.dot(table_low, high, preferred_element_type=jnp.float32)
    return total + jnp.dot(table_high, low, preferred_element_type=jnp.float32)


def spectral_kernel(
    views, pencils, chunks,
    sent, recorded, weight, turn_high, turn_low, back_high, back_low, picks, out, stacked,
    landed, high, low, product, terms, inverse,
    sent_sem, landed_sem, kept_sem, view_send, view_recv, back_send, back_recv, back_kept,
    share_send, share_recv, share_kept,
):
    view, me = lax.axis_index("view"), lax.axis_index("pencil")
    lines, nz, half = stacked.shape[2], weight.shape[2], weight.shape[3]
    rows = out.shape[2]
    mine = pl.ds(pl.multiple_of(me * rows, rows), rows)
    step = 2 - landed.shape[2] % 2

    barrier = pltpu.get_barrier_semaphore()

    @pl.loop(1, pencils)
    def _(d):
        pl.semaphore_signal(barrier, inc=1, device_id=(view, lax.rem(me + d, pencils)), device_id_type=MESH)

    @pl.loop(1, views)
    def _(d):
        pl.semaphore_signal(barrier, inc=1, device_id=(lax.rem(view + d, views), me), device_id_type=MESH)

    pl.semaphore_wait(barrier, pencils - 1 + views - 1)

    def forward(j, d):
        to = lax.rem(me + d, pencils)
        return pltpu.make_async_remote_copy(
            src_ref=sent.at[:, to, j], dst_ref=landed.at[j, :, :, me],
            send_sem=sent_sem.at[j, d], recv_sem=landed_sem.at[j, d],
            device_id=(view, to), device_id_type=MESH,
        )

    def kept(j):
        return pltpu.make_async_copy(sent.at[:, me, j], landed.at[j, :, :, me], kept_sem.at[j])

    def share(d):
        to = lax.rem(view + d, views)
        theirs = pl.ds(pl.multiple_of(to * lines, lines), lines)
        return pltpu.make_async_remote_copy(
            src_ref=recorded.at[0, :, theirs, :], dst_ref=stacked.at[view],
            send_sem=share_send.at[d], recv_sem=share_recv.at[d],
            device_id=(to, me), device_id_type=MESH,
        )

    def share_own():
        ours = pl.ds(pl.multiple_of(view * lines, lines), lines)
        return pltpu.make_async_copy(recorded.at[0, :, ours, :], stacked.at[view], share_kept)

    def across(j, d):
        to = lax.rem(view + d, views)
        return pltpu.make_async_remote_copy(
            src_ref=product.at[j, to], dst_ref=terms.at[j, d],
            send_sem=view_send.at[j, d], recv_sem=view_recv.at[j, d],
            device_id=(to, me), device_id_type=MESH,
        )

    def backward(j, d):
        to = lax.rem(me + d, pencils)
        theirs = pl.ds(pl.multiple_of(to * rows, rows), rows)
        return pltpu.make_async_remote_copy(
            src_ref=inverse.at[j, theirs, :], dst_ref=out.at[j, me],
            send_sem=back_send.at[j, d], recv_sem=back_recv.at[j, d],
            device_id=(view, to), device_id_type=MESH,
        )

    def back_own(j):
        return pltpu.make_async_copy(inverse.at[j, mine, :], out.at[j, me], back_kept.at[j])

    @pl.loop(0, chunks)
    def _(j):
        @pl.loop(1, pencils)
        def _(d):
            forward(j, d).start()

        kept(j).start()

    @pl.loop(1, views)
    def _(d):
        share(d).start()

    share_own().start()

    def finish(j):
        total = product[j, view]
        for d in range(1, views):
            across(j, d).wait_recv()
            total = total + terms[j, d]
        inverse[j] = thrice(back_high[...], back_low[...], total)

        @pl.loop(1, pencils)
        def _(d):
            backward(j, d).start()

        back_own(j).start()

    @pl.loop(0, chunks)
    def _(j):
        @pl.loop(1, pencils)
        def _(d):
            forward(j, d).wait_recv()

        kept(j).wait()

        for r in range(0, landed.shape[2], step):
            field = jnp.concatenate([
                jnp.concatenate([landed[j, c, r + i].reshape(nz, half) for i in range(step)], axis=1)
                for c in range(2)
            ], axis=0)
            spectrum = thrice(turn_high[...], turn_low[...], field)
            factor = jnp.concatenate([weight[j, r + i] for i in range(step)], axis=1)
            columns = slice(r * half, (r + step) * half)
            for c in range(2):
                part = spectrum[c * nz:(c + 1) * nz] * factor
                coarse = part.astype(jnp.bfloat16)
                high[c * nz:(c + 1) * nz, columns] = coarse
                low[c * nz:(c + 1) * nz, columns] = (part - coarse.astype(jnp.float32)).astype(jnp.bfloat16)

        @pl.loop(1, views + 1)
        def _(d):
            to = lax.rem(view + d, views)
            moved = jnp.dot(high[...], picks[to], preferred_element_type=jnp.float32)
            product[j, to] = moved + jnp.dot(low[...], picks[to], preferred_element_type=jnp.float32)

            @pl.when(d < views)
            def _():
                across(j, d).start()

        @pl.when(j > 0)
        def _():
            finish(j - 1)

    finish(chunks - 1)

    @pl.loop(0, chunks)
    def _(j):
        @pl.loop(1, pencils)
        def _(d):
            forward(j, d).wait_send()
            backward(j, d).wait()

        @pl.loop(1, views)
        def _(d):
            across(j, d).wait_send()

        back_own(j).wait()

    @pl.loop(1, views)
    def _(d):
        share(d).wait()

    share_own().wait()


def spectral(sent, recorded, weight, turn, back):
    views = lax.axis_size("view")
    _, pencils, chunks, block, depth, half = sent.shape
    whole, dma = pl.BlockSpec(memory_space=pltpu.VMEM), pltpu.SemaphoreType.DMA
    anywhere = pl.BlockSpec(memory_space=pl.ANY)
    total, quarter, lines = turn.shape[0], half // views, recorded.shape[2] // views
    lanes = block * quarter
    source, target = jnp.arange(block * half), jnp.arange(lanes)
    target = target // quarter * half + target % quarter
    target = target[None, :] + jnp.arange(views)[:, None] * quarter
    picks = (source[None, :, None] == target[:, None, :]).astype(jnp.bfloat16)
    return pl.pallas_call(
        functools.partial(spectral_kernel, views, pencils, chunks),
        out_shape=(
            jax.ShapeDtypeStruct((chunks, pencils, 2 * depth, lanes), jnp.float32),
            jax.ShapeDtypeStruct((views, depth, lines, recorded.shape[3]), jnp.float32),
        ),
        in_specs=[anywhere] * 2 + [whole] * 6,
        out_specs=(anywhere, anywhere),
        scratch_shapes=[
            pltpu.VMEM((chunks, 2, block, pencils, depth, half), jnp.float32),
            pltpu.VMEM((total, block * half), jnp.bfloat16),
            pltpu.VMEM((total, block * half), jnp.bfloat16),
            pltpu.VMEM((chunks, views, total, lanes), jnp.float32),
            pltpu.VMEM((chunks, views, total, lanes), jnp.float32),
            pltpu.VMEM((chunks, total, lanes), jnp.float32),
            dma((chunks, pencils)), dma((chunks, pencils)), dma((chunks,)),
            dma((chunks, views)), dma((chunks, views)),
            dma((chunks, pencils)), dma((chunks, pencils)), dma((chunks,)),
            dma((views,)), dma((views,)), dma,
        ],
        compiler_params=pltpu.CompilerParams(
            collective_id=0, has_side_effects=True, vmem_limit_bytes=60 << 20,
        ),
        cost_estimate=pl.CostEstimate(flops=10 ** 10, bytes_accessed=1 << 25, transcendentals=0),
    )(sent, recorded, weight, *parts_of(turn), *parts_of(back), picks)


def mirrored_weights(weights, half, chunks):
    pencils = lax.axis_size("pencil")
    nz, block, _ = weights.shape
    rows = block // chunks
    mirror = [(i, pencils - 1 - i) for i in range(pencils)]
    wrapped = [(i, (pencils - i) % pencils) for i in range(pencils)]
    positions, lanes = jnp.arange(nz), jnp.arange(half)
    flip_z = (positions[:, None] == (nz - positions[None, :]) % nz).astype(jnp.float32)
    flip_x = 0.5 * (lanes[:, None] == half - lanes[None, :]).astype(jnp.float32)
    share = jnp.where(lanes == 0, 1.0, 0.5)
    result = []
    for j in range(chunks):
        high = block - j * rows + 1
        if j == 0:
            upper = jnp.concatenate([weights[:, high - rows:high - 1, half:], weights[:, :1, half:]], axis=1)
        else:
            upper = weights[:, high - rows:high, half:]
        facing = mix("zrl,lx->rzx", jnp.flip(upper, axis=1), flip_x)
        facing = mix("zk,rzx->rkx", flip_z, facing)
        if j == 0:
            edge = lax.ppermute(facing[0], "pencil", wrapped)
        facing = lax.ppermute(facing, "pencil", mirror)
        if j == 0:
            facing = jnp.concatenate([edge[None], facing[1:]], axis=0)
        own = weights[:, j * rows:(j + 1) * rows, :half] * share
        result.append(own.transpose(1, 0, 2) + facing)
    return jnp.stack(result)


def nyquist_of(slab, weights, half, table_to, turn_z, back_z, table_from):
    signs = 1.0 - 2.0 * (jnp.arange(slab.shape[2]) % 2).astype(jnp.float32)
    depth, ny = slab.shape[:2]
    pencils = lax.axis_size("pencil")
    line = mix("dky,zy->zdk", table_to, jnp.sum(slab * signs, axis=-1))
    line = line.reshape(depth * 2, pencils, ny // pencils).swapaxes(0, 1)
    line = lax.all_to_all(line, "pencil", split_axis=0, concat_axis=0, tiled=True)
    line = line.reshape(pencils * depth, 2, ny // pencils)
    line = mix("dckz,zcy->dky", turn_z, line) * weights[:, :, half]
    line = mix("dczk,cky->zdy", back_z, line)
    line = line.reshape(pencils, depth * 2, ny // pencils)
    line = lax.all_to_all(line, "pencil", split_axis=0, concat_axis=0, tiled=True)
    line = line.reshape(pencils, depth, 2, ny // pencils)
    return mix("pzcb,cypb->zy", line, table_from)


def joined_of(recorded, weights):
    slab = recorded[0]
    views, pencils = lax.axis_size("view"), lax.axis_size("pencil")
    view = lax.axis_index("view")
    depth, ny, nx = slab.shape
    nz, block = weights.shape[:2]
    half, lines = nx // 2, ny // views
    quarter = half // views
    chunks = max(1, block * quarter // 256)
    rows = block // chunks
    halves = mirrored_weights(weights, half, chunks)

    to_view = lax.rem(view + jnp.arange(views, dtype=jnp.int32), views)
    source_view = lax.rem(view - jnp.arange(views, dtype=jnp.int32) + views, views)

    def spots(blocks, size):
        return (blocks[:, None] * size + jnp.arange(size, dtype=jnp.int32)[None, :]).reshape(-1)

    all_x, all_y = jnp.arange(nx, dtype=jnp.int32), jnp.arange(ny, dtype=jnp.int32)
    all_z = jnp.arange(nz, dtype=jnp.int32)
    cos_x, sin_x = turns(jnp.arange(half, dtype=jnp.int32), all_x, nx)
    rolled = mix("zyx,ckx->zcyk", slab, jnp.stack([cos_x, -sin_x]))
    cos_y, sin_y = turns(all_y, all_y, ny)
    piece = mix("dcky,zcyx->dkzx", rotation(cos_y, sin_y), rolled)
    piece = piece.reshape(2, pencils, chunks, rows, depth, half)

    cos_z, sin_z = turns(all_z, all_z, nz)
    turn_z, back_z = rotation(cos_z, sin_z), rotation(cos_z, -sin_z)
    turn = turn_z.transpose(0, 2, 1, 3).reshape(2 * nz, 2 * nz)
    back = back_z.reshape(2, 2, pencils, depth, nz).transpose(2, 0, 3, 1, 4).reshape(2 * nz, 2 * nz)
    cos_v, sin_v = turns(spots(to_view, lines), all_y, ny)
    back_y = rotation(cos_v, -sin_v).reshape(2, 2, views, lines, pencils, chunks, rows)
    edge = nyquist_of(
        slab, weights, half, jnp.stack([cos_y, -sin_y]), turn_z, back_z,
        jnp.stack([cos_v, -sin_v]).reshape(2, ny, pencils, block),
    ).reshape(depth, views, lines)
    got, stacked = spectral(piece, recorded, halves, turn, back)
    got = got.reshape(chunks, pencils, 2, depth, rows, quarter)
    spread = mix("jpczrx,dcvypjr->vzxdy", got, back_y)
    spread = spread.reshape(views, depth * quarter, 2 * lines)
    parts = [
        jnp.concatenate([spread[d], flat_rows(edge[:, d], 2 * lines)], axis=0)
        for d in range(views)
    ]
    parts = exchange(parts, "view")
    main = depth * quarter
    line = sum(part[main:].reshape(-1)[:depth * lines] for part in parts).reshape(depth, lines)
    spread = jnp.stack([part[:main].reshape(depth, quarter, 2, lines) for part in parts])
    scale = 1.0 / float(nz * ny * nx)
    waves = spots(source_view, quarter)
    cos_x, sin_x = turns(waves, all_x, nx)
    weight = jnp.where(waves == 0, scale, 2.0 * scale)[:, None]
    table = jnp.stack([cos_x * weight, -sin_x * weight]).reshape(2, views, quarter, nx)
    signs = 1.0 - 2.0 * (all_x % 2).astype(jnp.float32)
    joined = mix("vzkcy,cvkx->zyx", spread, table) + line[:, :, None] * (signs * scale)
    return joined, stacked


def body(recorded, spectral_weight, psf_taps):
    view_count = lax.axis_size("view")
    joined_volume, stacked = joined_of(recorded, spectral_weight[0])
    kernels = psf_taps / jnp.sum(psf_taps, axis=-1, keepdims=True)
    margin = kernels.shape[-1] // 2
    depth, rows, length = joined_volume.shape
    blur_z = band(kernels[:, 0], depth, depth + 2 * margin, 0)
    blur_y = band(kernels[:, 1], rows, rows + 2 * margin, 0)
    blur_x = band(kernels[:, 2], length, length, margin)
    local = 0.1 + jax.nn.softplus(joined_volume)
    for repeat in range(ITERS):
        padded = padded_2(local, (("view", 1), ("pencil", 0)), margin)
        field = mix("vza,abx->vzbx", blur_z, padded)
        field = mix("vyb,vzbx->vzyx", blur_y, field)
        ratio = stacked / mix("vzyx,vcx->vzyc", field, blur_x)
        field = mix("vzyc,vcx->vzyx", ratio, blur_x)
        field = mix("vyb,vzyx->vzbx", blur_y, field)
        total = mix("vza,vzbx->abx", blur_z, field)
        total = folded(folded(total, "pencil", 0, margin), "view", 1, margin)
        local = local * total / view_count
    return (joined_volume, local)


def solution(mesh):
    return jax.shard_map(
        body,
        mesh=mesh,
        in_specs=(P("view", "pencil", None, None), P("view", None, "pencil", None), P()),
        out_specs=(P("pencil", "view", None), P("pencil", "view", None)),
        check_vma=False,
    )
```

```python
import functools
import math

import jax
import jax.numpy as jnp
from jax import lax
from jax.experimental import pallas as pl
from jax.experimental.pallas import tpu as pltpu
from jax.sharding import PartitionSpec as P

ITERS = 2
MESH = pl.DeviceIdType.MESH


def mix(form, left, right):
    return jnp.einsum(form, left, right, precision=lax.Precision.HIGH)


def turns(first, second, length):
    product = first[:, None] * second[None, :] % length
    phases = product.astype(jnp.float32) * (2.0 * math.pi / length)
    return (jnp.cos(phases), jnp.sin(phases))


def rotation(cos, sin):
    return jnp.stack([jnp.stack([cos, sin]), jnp.stack([-sin, cos])])


def exchange(parts, axis):
    count = len(parts)
    got = [parts[0]]
    for step in range(1, count):
        pairs = [(i, (i + step) % count) for i in range(count)]
        got.append(lax.ppermute(parts[step], axis, pairs))
    return got


def flat_rows(value, width):
    flat = value.reshape(-1)
    rest = -flat.shape[0] % width
    return jnp.pad(flat, (0, rest)).reshape(-1, width)


def thrice_right(value, table_high, table_low):
    high = value.astype(jnp.bfloat16)
    low = (value - high.astype(jnp.float32)).astype(jnp.bfloat16)
    total = jnp.dot(high, table_high, preferred_element_type=jnp.float32)
    total += jnp.dot(high, table_low, preferred_element_type=jnp.float32)
    return total + jnp.dot(low, table_high, preferred_element_type=jnp.float32)


def ratio_kernel(
    taps, field, recorded, in_high, in_low, right_high, right_low, left_high, left_low, out_high, out_low,
    total, back,
):
    depth, lines, length = recorded.shape
    view, base = pl.program_id(0), pl.program_id(1) * depth
    count = taps.shape[1]
    weights = [taps[view, t] for t in range(count)]

    @pl.when((view == 0) & (base == 0))
    def _():
        @pl.loop(0, total.shape[0])
        def _(z):
            total[z] = jnp.zeros(total.shape[1:], jnp.float32)

    slices = []
    for z in range(depth):
        value = weights[0] * field[base + z]
        for t in range(1, count):
            value = value + weights[t] * field[base + z + t]
        slices.append(thrice(in_high[...], in_low[...], value))
    blurred = jnp.concatenate(slices, axis=0)
    blurred = thrice_right(blurred, right_high[...], right_low[...])
    ratio = recorded[...].reshape(depth * lines, length) / blurred
    ratio = thrice_right(ratio, left_high[...], left_low[...])
    for z in range(depth):
        back[z] = thrice(out_high[...], out_low[...], ratio[z * lines:(z + 1) * lines])
    for z in range(depth + count - 1):
        value = total[base + z]
        for t in range(max(0, z - depth + 1), min(count, z + 1)):
            value = value + weights[t] * back[z - t]
        total[base + z] = value


def corrections(padded, stacked, taps_z, blur_y, blur_x):
    views, depth, lines, length = stacked.shape
    tile = math.gcd(8, depth)
    tables = []
    for table in (blur_y, blur_x.swapaxes(1, 2), blur_x, blur_y.swapaxes(1, 2)):
        tables.extend(parts_of(table))
    whole = pl.BlockSpec(padded.shape, lambda v, z: (0, 0, 0))
    return pl.pallas_call(
        ratio_kernel,
        grid=(views, depth // tile),
        out_shape=jax.ShapeDtypeStruct(padded.shape, jnp.float32),
        in_specs=[
            pl.BlockSpec(memory_space=pltpu.SMEM), whole,
            pl.BlockSpec((None, tile, lines, length), lambda v, z: (v, z, 0, 0)),
        ] + [pl.BlockSpec((None,) + table.shape[1:], lambda v, z: (v, 0, 0)) for table in tables],
        out_specs=whole,
        scratch_shapes=[pltpu.VMEM((tile,) + padded.shape[1:], jnp.float32)],
        compiler_params=pltpu.CompilerParams(vmem_limit_bytes=40 << 20),
        cost_estimate=pl.CostEstimate(flops=2 * 10 ** 10, bytes_accessed=1 << 25, transcendentals=0),
    )(taps_z, padded, stacked, *tables)


def swap(axis, place, lower_pair, upper_pair, sems):
    index, count = lax.axis_index(axis), lax.axis_size(axis)
    lower = pltpu.make_async_remote_copy(
        src_ref=lower_pair[0], dst_ref=lower_pair[1], send_sem=sems.at[place, 0], recv_sem=sems.at[place, 1],
        device_id={axis: index - 1}, device_id_type=MESH,
    )
    upper = pltpu.make_async_remote_copy(
        src_ref=upper_pair[0], dst_ref=upper_pair[1], send_sem=sems.at[place, 2], recv_sem=sems.at[place, 3],
        device_id={axis: index + 1}, device_id_type=MESH,
    )

    @pl.when(index > 0)
    def _():
        lower.start()

    @pl.when(index < count - 1)
    def _():
        upper.start()

    def wait():
        @pl.when(index > 0)
        def _():
            lower.wait_send()
            upper.wait_recv()

        @pl.when(index == 0)
        def _():
            upper_pair[1][...] = jnp.zeros(upper_pair[1].shape, jnp.float32)

        @pl.when(index < count - 1)
        def _():
            upper.wait_send()
            lower.wait_recv()

        @pl.when(index == count - 1)
        def _():
            lower_pair[1][...] = jnp.zeros(lower_pair[1].shape, jnp.float32)

    return wait


def edges_kernel(width, fold, pad, *refs):
    refs = list(refs)
    total = refs.pop(0) if fold else None
    local = refs.pop(0) if pad else None
    result = refs.pop(0) if fold else None
    padded = refs.pop(0) if pad else None
    from_z, held, to_y, from_y, sems = refs
    shape = local.shape if pad else result.shape
    depth, lines = shape[0], shape[1]
    top, bottom = slice(0, width), slice(lines - width, lines)

    barrier = pltpu.get_barrier_semaphore()
    for axis in ("view", "pencil"):
        index, count = lax.axis_index(axis), lax.axis_size(axis)
        for near, there in ((index - 1, index > 0), (index + 1, index < count - 1)):
            @pl.when(there)
            def _(axis=axis, near=near):
                pl.semaphore_signal(barrier, inc=1, device_id={axis: near}, device_id_type=MESH)
    peers = 0
    for axis in ("view", "pencil"):
        index, count = lax.axis_index(axis), lax.axis_size(axis)
        peers = peers + jnp.minimum(index, 1) + jnp.minimum(count - 1 - index, 1)
    pl.semaphore_wait(barrier, peers)

    if fold:
        wait = swap(
            "pencil", 0, (total.at[:width], from_z.at[1]),
            (total.at[depth + width:], from_z.at[0]), sems,
        )

        @pl.loop(0, depth)
        def _(z):
            held[z] = total[width + z]

        wait()
        for i in range(width):
            held[i] = held[i] + from_z[0, i]
            held[depth - width + i] = held[depth - width + i] + from_z[1, i]

        @pl.loop(0, depth)
        def _(z):
            to_y[0, 0, z] = held[z, :width]
            to_y[0, 1, z] = held[z, lines + width:]

        wait = swap(
            "view", 1, (to_y.at[0, 0], from_y.at[0, 1]), (to_y.at[0, 1], from_y.at[0, 0]), sems,
        )

        @pl.loop(0, depth)
        def _(z):
            result[z] = held[z, width:lines + width]

        wait()

        @pl.loop(0, depth)
        def _(z):
            result[z, top] = result[z, top] + from_y[0, 0, z]
            result[z, bottom] = result[z, bottom] + from_y[0, 1, z]
            if pad:
                result[z] = local[z] * result[z] * (1.0 / lax.axis_size("view"))

    if pad:
        value = result if fold else local

        @pl.loop(0, depth)
        def _(z):
            to_y[1, 0, z] = value[z, top]
            to_y[1, 1, z] = value[z, bottom]

        wait = swap(
            "view", 2, (to_y.at[1, 0], from_y.at[1, 1]), (to_y.at[1, 1], from_y.at[1, 0]), sems,
        )

        @pl.loop(0, depth)
        def _(z):
            padded[width + z, width:lines + width] = value[z]

        wait()

        @pl.loop(0, depth)
        def _(z):
            padded[width + z, :width] = from_y[1, 0, z]
            padded[width + z, lines + width:] = from_y[1, 1, z]

        wait = swap(
            "pencil", 3, (padded.at[width:2 * width], padded.at[depth + width:]),
            (padded.at[depth:depth + width], padded.at[:width]), sems,
        )
        wait()


def edges(width, number, total=None, local=None):
    fold, pad = total is not None, local is not None
    depth, lines, length = local.shape if pad else (total.shape[0] - 2 * width, total.shape[1] - 2 * width, total.shape[2])
    wide = lines + 2 * width
    whole, vector = pl.BlockSpec(memory_space=pltpu.VMEM), jnp.float32
    shapes = []
    if fold:
        shapes.append(jax.ShapeDtypeStruct((depth, lines, length), vector))
    if pad:
        shapes.append(jax.ShapeDtypeStruct((depth + 2 * width, wide, length), vector))
    given = [value for value in (total, local) if value is not None]
    return pl.pallas_call(
        functools.partial(edges_kernel, width, fold, pad),
        out_shape=shapes,
        in_specs=[whole] * len(given),
        out_specs=[whole] * len(shapes),
        scratch_shapes=[
            pltpu.VMEM((2, width, wide, length), vector),
            pltpu.VMEM((depth, wide, length), vector),
            pltpu.VMEM((2, 2, depth, width, length), vector),
            pltpu.VMEM((2, 2, depth, width, length), vector),
            pltpu.SemaphoreType.DMA((4, 4)),
        ],
        compiler_params=pltpu.CompilerParams(
            collective_id=number, has_side_effects=True, vmem_limit_bytes=24 << 20,
        ),
    )(*given)


def band(taps, rows, columns, shift):
    offset = jnp.arange(columns)[None, :] - jnp.arange(rows)[:, None] + shift
    total = jnp.zeros((taps.shape[0], rows, columns), jnp.float32)
    for t in range(taps.shape[1]):
        total = total + jnp.where(offset == t, taps[:, t, None, None], 0.0)
    return total


def parts_of(value):
    high = lax.reduce_precision(value, 8, 7)
    return high.astype(jnp.bfloat16), (value - high).astype(jnp.bfloat16)


def thrice(table_high, table_low, value):
    high = value.astype(jnp.bfloat16)
    low = (value - high.astype(jnp.float32)).astype(jnp.bfloat16)
    total = jnp.dot(table_high, high, preferred_element_type=jnp.float32)
    total += jnp.dot(table_low, high, preferred_element_type=jnp.float32)
    return total + jnp.dot(table_high, low, preferred_element_type=jnp.float32)


def spectral_kernel(
    views, pencils, chunks,
    sent, recorded, weight, turn_high, turn_low, back_high, back_low, picks, out, stacked,
    landed, high, low, product, terms, inverse,
    sent_sem, landed_sem, kept_sem, view_send, view_recv, back_send, back_recv, back_kept,
    share_send, share_recv, share_kept,
):
    view, me = lax.axis_index("view"), lax.axis_index("pencil")
    lines, nz, half = stacked.shape[2], weight.shape[2], weight.shape[3]
    rows = out.shape[2]
    mine = pl.ds(pl.multiple_of(me * rows, rows), rows)
    step = 2 - landed.shape[2] % 2

    barrier = pltpu.get_barrier_semaphore()

    @pl.loop(1, pencils)
    def _(d):
        pl.semaphore_signal(barrier, inc=1, device_id=(view, lax.rem(me + d, pencils)), device_id_type=MESH)

    @pl.loop(1, views)
    def _(d):
        pl.semaphore_signal(barrier, inc=1, device_id=(lax.rem(view + d, views), me), device_id_type=MESH)

    pl.semaphore_wait(barrier, pencils - 1 + views - 1)

    def forward(j, d):
        to = lax.rem(me + d, pencils)
        return pltpu.make_async_remote_copy(
            src_ref=sent.at[:, to, j], dst_ref=landed.at[j, :, :, me],
            send_sem=sent_sem.at[j, d], recv_sem=landed_sem.at[j, d],
            device_id=(view, to), device_id_type=MESH,
        )

    def kept(j):
        return pltpu.make_async_copy(sent.at[:, me, j], landed.at[j, :, :, me], kept_sem.at[j])

    def share(d):
        to = lax.rem(view + d, views)
        theirs = pl.ds(pl.multiple_of(to * lines, lines), lines)
        return pltpu.make_async_remote_copy(
            src_ref=recorded.at[0, :, theirs, :], dst_ref=stacked.at[view],
            send_sem=share_send.at[d], recv_sem=share_recv.at[d],
            device_id=(to, me), device_id_type=MESH,
        )

    def share_own():
        ours = pl.ds(pl.multiple_of(view * lines, lines), lines)
        return pltpu.make_async_copy(recorded.at[0, :, ours, :], stacked.at[view], share_kept)

    def across(j, d):
        to = lax.rem(view + d, views)
        return pltpu.make_async_remote_copy(
            src_ref=product.at[j, to], dst_ref=terms.at[j, d],
            send_sem=view_send.at[j, d], recv_sem=view_recv.at[j, d],
            device_id=(to, me), device_id_type=MESH,
        )

    def backward(j, d):
        to = lax.rem(me + d, pencils)
        theirs = pl.ds(pl.multiple_of(to * rows, rows), rows)
        return pltpu.make_async_remote_copy(
            src_ref=inverse.at[j, theirs, :], dst_ref=out.at[j, me],
            send_sem=back_send.at[j, d], recv_sem=back_recv.at[j, d],
            device_id=(view, to), device_id_type=MESH,
        )

    def back_own(j):
        return pltpu.make_async_copy(inverse.at[j, mine, :], out.at[j, me], back_kept.at[j])

    @pl.loop(0, chunks)
    def _(j):
        @pl.loop(1, pencils)
        def _(d):
            forward(j, d).start()

        kept(j).start()

    @pl.loop(1, views)
    def _(d):
        share(d).start()

    share_own().start()

    def finish(j):
        total = product[j, view]
        for d in range(1, views):
            across(j, d).wait_recv()
            total = total + terms[j, d]
        inverse[j] = thrice(back_high[...], back_low[...], total)

        @pl.loop(1, pencils)
        def _(d):
            backward(j, d).start()

        back_own(j).start()

    @pl.loop(0, chunks)
    def _(j):
        @pl.loop(1, pencils)
        def _(d):
            forward(j, d).wait_recv()

        kept(j).wait()

        for r in range(0, landed.shape[2], step):
            field = jnp.concatenate([
                jnp.concatenate([landed[j, c, r + i].reshape(nz, half) for i in range(step)], axis=1)
                for c in range(2)
            ], axis=0)
            spectrum = thrice(turn_high[...], turn_low[...], field)
            factor = jnp.concatenate([weight[j, r + i] for i in range(step)], axis=1)
            columns = slice(r * half, (r + step) * half)
            for c in range(2):
                part = spectrum[c * nz:(c + 1) * nz] * factor
                coarse = part.astype(jnp.bfloat16)
                high[c * nz:(c + 1) * nz, columns] = coarse
                low[c * nz:(c + 1) * nz, columns] = (part - coarse.astype(jnp.float32)).astype(jnp.bfloat16)

        @pl.loop(1, views + 1)
        def _(d):
            to = lax.rem(view + d, views)
            moved = jnp.dot(high[...], picks[to], preferred_element_type=jnp.float32)
            product[j, to] = moved + jnp.dot(low[...], picks[to], preferred_element_type=jnp.float32)

            @pl.when(d < views)
            def _():
                across(j, d).start()

        @pl.when(j > 0)
        def _():
            finish(j - 1)

    finish(chunks - 1)

    @pl.loop(0, chunks)
    def _(j):
        @pl.loop(1, pencils)
        def _(d):
            forward(j, d).wait_send()
            backward(j, d).wait()

        @pl.loop(1, views)
        def _(d):
            across(j, d).wait_send()

        back_own(j).wait()

    @pl.loop(1, views)
    def _(d):
        share(d).wait()

    share_own().wait()


def spectral(sent, recorded, weight, turn, back):
    views = lax.axis_size("view")
    _, pencils, chunks, block, depth, half = sent.shape
    whole, dma = pl.BlockSpec(memory_space=pltpu.VMEM), pltpu.SemaphoreType.DMA
    anywhere = pl.BlockSpec(memory_space=pl.ANY)
    total, quarter, lines = turn.shape[0], half // views, recorded.shape[2] // views
    lanes = block * quarter
    source, target = jnp.arange(block * half), jnp.arange(lanes)
    target = target // quarter * half + target % quarter
    target = target[None, :] + jnp.arange(views)[:, None] * quarter
    picks = (source[None, :, None] == target[:, None, :]).astype(jnp.bfloat16)
    return pl.pallas_call(
        functools.partial(spectral_kernel, views, pencils, chunks),
        out_shape=(
            jax.ShapeDtypeStruct((chunks, pencils, 2 * depth, lanes), jnp.float32),
            jax.ShapeDtypeStruct((views, depth, lines, recorded.shape[3]), jnp.float32),
        ),
        in_specs=[anywhere] * 2 + [whole] * 6,
        out_specs=(anywhere, anywhere),
        scratch_shapes=[
            pltpu.VMEM((chunks, 2, block, pencils, depth, half), jnp.float32),
            pltpu.VMEM((total, block * half), jnp.bfloat16),
            pltpu.VMEM((total, block * half), jnp.bfloat16),
            pltpu.VMEM((chunks, views, total, lanes), jnp.float32),
            pltpu.VMEM((chunks, views, total, lanes), jnp.float32),
            pltpu.VMEM((chunks, total, lanes), jnp.float32),
            dma((chunks, pencils)), dma((chunks, pencils)), dma((chunks,)),
            dma((chunks, views)), dma((chunks, views)),
            dma((chunks, pencils)), dma((chunks, pencils)), dma((chunks,)),
            dma((views,)), dma((views,)), dma,
        ],
        compiler_params=pltpu.CompilerParams(
            collective_id=0, has_side_effects=True, vmem_limit_bytes=60 << 20,
        ),
        cost_estimate=pl.CostEstimate(flops=10 ** 10, bytes_accessed=1 << 25, transcendentals=0),
    )(sent, recorded, weight, *parts_of(turn), *parts_of(back), picks)


def mirrored_weights(slab, weights, half, chunks):
    pencils = lax.axis_size("pencil")
    nz, block, _ = weights.shape
    rows = block // chunks
    mirror = [(i, pencils - 1 - i) for i in range(pencils)]
    wrapped = [(i, (pencils - i) % pencils) for i in range(pencils)]
    positions, lanes = jnp.arange(nz), jnp.arange(half)
    flip_z = (positions[:, None] == (nz - positions[None, :]) % nz).astype(jnp.float32)
    flip_x = 0.5 * (lanes[:, None] == half - lanes[None, :]).astype(jnp.float32)
    share = jnp.where(lanes == 0, 1.0, 0.5)
    sent = []
    for j in range(chunks):
        high = block - j * rows + 1
        if j == 0:
            upper = jnp.concatenate([weights[:, high - rows:high - 1, half:], weights[:, :1, half:]], axis=1)
        else:
            upper = weights[:, high - rows:high, half:]
        facing = mix("zrl,lx->rzx", jnp.flip(upper, axis=1), flip_x)
        sent.append(mix("zk,rzx->rkx", flip_z, facing))
    slab, *sent = lax.optimization_barrier((slab, *sent))
    edge = lax.ppermute(sent[0][0], "pencil", wrapped)
    result = []
    for j in range(chunks):
        facing = lax.ppermute(sent[j], "pencil", mirror)
        if j == 0:
            facing = jnp.concatenate([edge[None], facing[1:]], axis=0)
        own = weights[:, j * rows:(j + 1) * rows, :half] * share
        result.append(own.transpose(1, 0, 2) + facing)
    return slab, jnp.stack(result)


def nyquist_of(slab, weights, half, table_to, turn_z, back_z, table_from):
    signs = 1.0 - 2.0 * (jnp.arange(slab.shape[2]) % 2).astype(jnp.float32)
    depth, ny = slab.shape[:2]
    pencils = lax.axis_size("pencil")
    line = mix("dky,zy->zdk", table_to, jnp.sum(slab * signs, axis=-1))
    line = line.reshape(depth * 2, pencils, ny // pencils).swapaxes(0, 1)
    line = lax.all_to_all(line, "pencil", split_axis=0, concat_axis=0, tiled=True)
    line = line.reshape(pencils * depth, 2, ny // pencils)
    line = mix("dckz,zcy->dky", turn_z, line) * weights[:, :, half]
    line = mix("dczk,cky->zdy", back_z, line)
    line = line.reshape(pencils, depth * 2, ny // pencils)
    line = lax.all_to_all(line, "pencil", split_axis=0, concat_axis=0, tiled=True)
    line = line.reshape(pencils, depth, 2, ny // pencils)
    return mix("pzcb,cypb->zy", line, table_from)


def joined_of(recorded, weights):
    slab = recorded[0]
    views, pencils = lax.axis_size("view"), lax.axis_size("pencil")
    view = lax.axis_index("view")
    depth, ny, nx = slab.shape
    nz, block = weights.shape[:2]
    half, lines = nx // 2, ny // views
    quarter = half // views
    chunks = max(1, block * quarter // 256)
    rows = block // chunks
    slab, halves = mirrored_weights(slab, weights, half, chunks)

    to_view = lax.rem(view + jnp.arange(views, dtype=jnp.int32), views)
    source_view = lax.rem(view - jnp.arange(views, dtype=jnp.int32) + views, views)

    def spots(blocks, size):
        return (blocks[:, None] * size + jnp.arange(size, dtype=jnp.int32)[None, :]).reshape(-1)

    all_x, all_y = jnp.arange(nx, dtype=jnp.int32), jnp.arange(ny, dtype=jnp.int32)
    all_z = jnp.arange(nz, dtype=jnp.int32)
    cos_x, sin_x = turns(jnp.arange(half, dtype=jnp.int32), all_x, nx)
    rolled = mix("zyx,ckx->zcyk", slab, jnp.stack([cos_x, -sin_x]))
    cos_y, sin_y = turns(all_y, all_y, ny)
    piece = mix("dcky,zcyx->dkzx", rotation(cos_y, sin_y), rolled)
    piece = piece.reshape(2, pencils, chunks, rows, depth, half)

    cos_z, sin_z = turns(all_z, all_z, nz)
    turn_z, back_z = rotation(cos_z, sin_z), rotation(cos_z, -sin_z)
    turn = turn_z.transpose(0, 2, 1, 3).reshape(2 * nz, 2 * nz)
    back = back_z.reshape(2, 2, pencils, depth, nz).transpose(2, 0, 3, 1, 4).reshape(2 * nz, 2 * nz)
    cos_v, sin_v = turns(spots(to_view, lines), all_y, ny)
    back_y = rotation(cos_v, -sin_v).reshape(2, 2, views, lines, pencils, chunks, rows)
    edge = nyquist_of(
        slab, weights, half, jnp.stack([cos_y, -sin_y]), turn_z, back_z,
        jnp.stack([cos_v, -sin_v]).reshape(2, ny, pencils, block),
    ).reshape(depth, views, lines)
    got, stacked = spectral(piece, recorded, halves, turn, back)
    got = got.reshape(chunks, pencils, 2, depth, rows, quarter)
    spread = mix("jpczrx,dcvypjr->vzxdy", got, back_y)
    spread = spread.reshape(views, depth * quarter, 2 * lines)
    parts = [
        jnp.concatenate([spread[d], flat_rows(edge[:, d], 2 * lines)], axis=0)
        for d in range(views)
    ]
    parts = exchange(parts, "view")
    main = depth * quarter
    line = sum(part[main:].reshape(-1)[:depth * lines] for part in parts).reshape(depth, lines)
    spread = jnp.stack([part[:main].reshape(depth, quarter, 2, lines) for part in parts])
    scale = 1.0 / float(nz * ny * nx)
    waves = spots(source_view, quarter)
    cos_x, sin_x = turns(waves, all_x, nx)
    weight = jnp.where(waves == 0, scale, 2.0 * scale)[:, None]
    table = jnp.stack([cos_x * weight, -sin_x * weight]).reshape(2, views, quarter, nx)
    signs = 1.0 - 2.0 * (all_x % 2).astype(jnp.float32)
    joined = mix("vzkcy,cvkx->zyx", spread, table) + line[:, :, None] * (signs * scale)
    return joined, stacked


def body(recorded, spectral_weight, psf_taps):
    view_count = lax.axis_size("view")
    joined_volume, stacked = joined_of(recorded, spectral_weight[0])
    kernels = psf_taps / jnp.sum(psf_taps, axis=-1, keepdims=True)
    margin = kernels.shape[-1] // 2
    depth, rows, length = joined_volume.shape
    blur_y = band(kernels[:, 1], rows, rows + 2 * margin, 0)
    blur_x = band(kernels[:, 2], length, length, margin)
    local = 0.1 + jax.nn.softplus(joined_volume)
    padded, = edges(margin, 1, local=local)
    for repeat in range(ITERS):
        total = corrections(padded, stacked, kernels[:, 0], blur_y, blur_x)
        if repeat < ITERS - 1:
            local, padded = edges(margin, 2, total=total, local=local)
        else:
            total, = edges(margin, 3, total=total)
            local = local * total / view_count
    return (joined_volume, local)


def solution(mesh):
    return jax.shard_map(
        body,
        mesh=mesh,
        in_specs=(P("view", "pencil", None, None), P("view", None, "pencil", None), P()),
        out_specs=(P("pencil", "view", None), P("pencil", "view", None)),
        check_vma=False,
    )
```
